32 devices in a mesh: blk: 8 (over z, y), pix: 4 (over x, core).
Axes of the slice: x: 2, y: 2, z: 4, core: 2. Of those that a mesh axis runs over, the one named last changes fastest.
Arguments:
- pixels: bfloat16 [32768, 224], P(('blk', 'pix')), may hold values from -6 to 6
- bundles: bfloat16 [16, 224, 64], P('blk'), may hold values from -0.375 to 0.375
- assign: int32 [32768, 1], P(('blk', 'pix')), may hold values from 0 to 15; in each aligned block of 1024 rows (0 to 1023, 1024 to 2047, ...) at most 128 rows name the same one
Outputs:
- abundances: float32 [32768, 64], P(('blk', 'pix'))
- residual_energy: float32 [8, 16], P('blk')
The draws below stay inside these ranges and needn't reach their ends.
Inputs may be any that keep to these rules, and one draw needn't show every extreme that they name: `assign`: among the 1024 rows of one device no bundle is named more than 128 times; in every draw some device names some bundle exactly 128 times; every bundle is named somewhere.
All inputs are finite; a program needn't handle non-finite values. Where the reference program divides by a largest or mean magnitude, that divisor is 1e-20 or more.
Results may differ from the reference program's by a relative error of at most 0.0003.
Values may be sent and summed in bfloat16 or wider, within the bound.
A program may use at most 64 MiB of HBM per device.

```python
import math
import jax
import jax.numpy as jnp
import numpy as np
from jax import lax

BANDS = 224
ENDMEMBERS = 64
ITERS = 8
PIX_DEV = 1024
BUNDLES = 16
CAP = 128
PIXELS = 32768
N_BLK = 8
N_PIX = 4


def shard_levels(key, extent, cuts, least, largest):
    def one(dim, parts):
        heights = jax.random.uniform(jax.random.fold_in(jax.random.fold_in(key, 6), dim), (parts,), jnp.float32, least / len(cuts), largest / len(cuts))
        return jnp.repeat(jnp.exp(heights), extent[dim] // parts).reshape((-1,) + (1,) * (len(extent) - dim - 1))

    loudness = one(*cuts[0])
    for cut in cuts[1:]:
        loudness = loudness * one(*cut)
    return loudness


def routed_block(own_key, own, number, rows, amount, top, most, skew):
    ranking = jax.random.permutation(own_key, amount)
    packed, common = shares(amount, rows * top, most, skew, True), shares(amount, rows * top, most, skew, False)
    places = jnp.arange(amount)

    def named(sizes, rotation):
        used = int((sizes > 0).sum())
        fixed = max(1, used // 4)
        passed = fixed + (places - fixed + rotation * (used - fixed)) % max(1, amount - fixed)
        return jnp.zeros((amount,), jnp.int32).at[ranking[jnp.where(places < fixed, places, passed)]].set(jnp.asarray(sizes, jnp.int32))

    sizes = jnp.where(number % 4 == 0, named(packed, number // 4), named(common, number - number // 4 - 1))
    mixed = jax.random.permutation(jax.random.fold_in(own, 3), amount)
    giver, receiver = mixed[0:amount // 2 * 2:2], mixed[1:amount // 2 * 2:2]
    room = jnp.minimum(sizes[giver] - 1, most - sizes[receiver]) // 2
    room = jnp.where((giver == ranking[0]) | (receiver == ranking[0]) | (sizes[receiver] == 0), 0, jnp.maximum(room, 0))
    passed = jax.random.randint(jax.random.fold_in(own, 4), (amount // 2,), 0, 1 << 20) % (room + 1)
    sizes = sizes.at[giver].add(-passed).at[receiver].add(passed)
    members = jnp.searchsorted(jnp.cumsum(sizes), jnp.arange(rows * top), side="right").astype(jnp.int32)
    table = members.reshape(top, rows).T
    table = table[jax.random.permutation(jax.random.fold_in(own, 1), rows)]
    rotation = jax.random.randint(jax.random.fold_in(own, 2), (rows, 1), 0, top)
    return jnp.take_along_axis(table, (jnp.arange(top)[None, :] + rotation) % top, axis=1)


def shares(amount, total, reach, slope, full):
    portions = [(1 << 20) // math.isqrt(grade ** slope) + 1 for grade in range(1, amount + 1)]
    largest = reach if full else min(reach, max(-(-total // amount), total * portions[0] // sum(portions)))
    least = 1 if total - largest >= amount - 1 else 0
    counts, rest = [largest] + [least] * (amount - 1), total - largest - least * (amount - 1)
    while rest > 0:
        movable = [i for i in range(1, amount) if counts[i] < largest] or [i for i in range(1, amount) if counts[i] < reach]
        mass, budget = sum([portions[i] for i in movable]), rest
        for i in movable:
            extra = min(reach - counts[i], max(1, budget * portions[i] // mass), rest)
            counts[i] = counts[i] + extra
            rest = rest - extra
    return np.array(counts)


def normal_values(rng, extent, scale, bound, split=(), held_as=jnp.bfloat16):
    values = scale * jax.random.normal(rng, extent, jnp.float32)
    if split:
        values = values * shard_levels(rng, extent, split, -0.22, 0.18)
    return jnp.clip(values, -bound, bound).astype(held_as)


def setup_inputs(seed: int = 0) -> dict:
    key_of = jax.random.split(jax.random.key(seed), 4)
    pixels = normal_values(key_of[0], (PIXELS, BANDS), 1.0, 6.0, ((0, 32),))
    bundles = normal_values(key_of[1], (BUNDLES, BANDS, ENDMEMBERS), BANDS ** -0.5, 0.375, ((0, 8),))
    assign_keys = jax.random.split(jax.random.fold_in(key_of[2], 1), PIXELS // PIX_DEV)
    assign_turns = jax.random.permutation(jax.random.fold_in(key_of[2], 3), PIXELS // PIX_DEV)
    assign = jax.vmap(lambda own, number: routed_block(jax.random.fold_in(key_of[2], 2), own, number, PIX_DEV, BUNDLES, 1, CAP, 1))(assign_keys, assign_turns).reshape((PIXELS, 1))
    return {"pixels": pixels, "bundles": bundles, "assign": assign}


sum_weight = 0.015625


def make_slots(assign, count, cap):
    labels = assign[:, 0].astype(jnp.int32)
    onehot = (labels[:, None] == jnp.arange(count, dtype=jnp.int32)[None, :]).astype(jnp.int32)
    ranked = jnp.sum(jnp.cumsum(onehot, axis=0) * onehot, axis=1) - 1
    return (labels * cap + ranked).astype(jnp.int32)


def solve_ref(blocks, spectra, gram, step):
    wide = spectra.astype(jnp.float32)
    target = jnp.einsum("nsb,nbm->nsm", blocks.astype(jnp.float32), wide, precision=lax.Precision.HIGHEST) + sum_weight

    def sweep(index, state):
        grad = jnp.einsum("nsm,nmk->nsk", state, gram, precision=lax.Precision.HIGHEST)
        return jnp.maximum(state - step[:, None, None] * (grad - target), 0.0)

    state = lax.fori_loop(0, ITERS, sweep, jnp.zeros_like(target))
    fitted = jnp.einsum("nsm,nbm->nsb", state, wide, precision=lax.Precision.HIGHEST)
    misfit = blocks.astype(jnp.float32) - fitted
    return state, jnp.sum(misfit * misfit, axis=-1)


def reference(pixels, bundles, assign):
    wide = bundles.astype(jnp.float32)
    gram = jnp.einsum("nbm,nbk->nmk", wide, wide, precision=lax.Precision.HIGHEST) + sum_weight
    step = 1.0 / jnp.max(jnp.sum(jnp.abs(gram), axis=2), axis=1)
    scale = BANDS * PIX_DEV * N_PIX / BUNDLES
    blocks_in = pixels.reshape(N_BLK * N_PIX, PIX_DEV, BANDS)
    labels_in = assign.reshape(N_BLK * N_PIX, PIX_DEV, 1)

    def per_block(item):
        values, labels = item
        slots = make_slots(labels, BUNDLES, CAP)
        flat = jnp.zeros((BUNDLES * CAP, BANDS), jnp.bfloat16).at[slots].set(values)
        valid = jnp.zeros((BUNDLES * CAP,), jnp.float32).at[slots].set(1.0).reshape(BUNDLES, CAP)
        state, misfit = solve_ref(flat.reshape(BUNDLES, CAP, BANDS), bundles, gram, step)
        chosen = state.reshape(BUNDLES * CAP, ENDMEMBERS)[slots]
        energy = jnp.sum(misfit * valid / scale, axis=1)
        return chosen, energy

    chosen, energy = lax.map(per_block, (blocks_in, labels_in))
    return chosen.reshape(PIXELS, ENDMEMBERS), jnp.sum(energy.reshape(N_BLK, N_PIX, BUNDLES), axis=1)
```

```python
import functools

import jax
import jax.numpy as jnp
from jax import lax
from jax.experimental import pallas as pl
from jax.experimental.pallas import tpu as pltpu
from jax.sharding import PartitionSpec as P

ITERS = 8
MESH = pl.DeviceIdType.MESH
LANES = 128
TILE = 256

sum_weight = 0.015625


def split(value):
    high = value.astype(jnp.bfloat16)
    low = (value - high.astype(jnp.float32)).astype(jnp.bfloat16)
    return high, low


def mask(cond):
    return jnp.where(cond, 1.0, 0.0).astype(jnp.bfloat16)


def dot(a, b, dims=((1,), (0,))):
    return lax.dot_general(a, b, (dims, ((), ())), preferred_element_type=jnp.float32)


def kernel(
    dims, label_ref, pix_hbm, bun_hbm, out_hbm, energy_ref,
    pix, own, spectra, slots, counts, pick, part, m_ref, c_ref, a_ref, packed, out, sums,
    local_sem, out_sem, send_sem, recv_sem, esend_sem, erecv_sem,
):
    n_blk, n_pix = dims
    me, my = lax.axis_index("blk"), lax.axis_index("pix")
    rows, bands = pix.shape
    owned, _, width = own.shape
    count = n_blk * owned
    cap = 2 * rows // count
    per = TILE // width
    groups = count // per
    packed_rows = groups * cap

    get_bun = pltpu.make_async_copy(bun_hbm, own, local_sem.at[0])
    get_pix = pltpu.make_async_copy(pix_hbm, pix, local_sem.at[1])
    get_bun.start()
    get_pix.start()

    barrier = pltpu.get_barrier_semaphore()
    for o in range(1, n_blk):
        pl.semaphore_signal(
            barrier, inc=1, device_id=(lax.rem(me + o, n_blk), my), device_id_type=MESH
        )
    for o in range(1, n_pix):
        pl.semaphore_signal(
            barrier, inc=1, device_id=(me, lax.rem(my + o, n_pix)), device_id_type=MESH
        )
    get_bun.wait()
    spectra[me] = jnp.concatenate([own[i] for i in range(owned)], axis=1)
    pl.semaphore_wait(barrier, n_blk + n_pix - 2)

    def bundle_copy(o, slot):
        return pltpu.make_async_remote_copy(
            src_ref=spectra.at[slot],
            dst_ref=spectra.at[slot],
            send_sem=send_sem.at[o],
            recv_sem=recv_sem.at[o],
            device_id=(lax.rem(me + o, n_blk), my),
            device_id_type=MESH,
        )

    for o in range(1, n_blk):
        bundle_copy(o, me).start()

    label = label_ref[...]
    kinds = lax.broadcasted_iota(jnp.int32, (count, TILE), 0)
    blocks = rows // TILE
    hot = [
        jnp.where(label[:, b * TILE:(b + 1) * TILE] == kinds, 1.0, 0.0) for b in range(blocks)
    ]
    upper = mask(
        lax.broadcasted_iota(jnp.int32, (TILE, TILE), 0)
        <= lax.broadcasted_iota(jnp.int32, (TILE, TILE), 1)
    )
    run = dot(jnp.concatenate(hot, axis=0).astype(jnp.bfloat16), upper)
    carry = jnp.zeros((count, 1), jnp.float32)
    ranks = []
    for b in range(blocks):
        here = run[b * count:(b + 1) * count]
        ranks.append(jnp.sum(hot[b] * (here + carry), axis=0, keepdims=True) - 1.0)
        carry = carry + here[:, TILE - 1:TILE]
    counts[...] = jnp.broadcast_to(carry, counts.shape)
    rank = jnp.concatenate(ranks, axis=1)
    shift = per.bit_length() - 1
    slot = label.astype(jnp.float32) * float(cap) + rank
    place = (label >> shift).astype(jnp.float32) * float(cap) + rank
    piece = (label & (per - 1)).astype(jnp.float32)

    get_pix.wait()
    step_rows = 512
    for s in range(count * cap // step_rows):
        index = lax.broadcasted_iota(jnp.int32, (step_rows, rows), 0) + s * step_rows
        chosen = mask(slot == index.astype(jnp.float32))
        slots[s * step_rows:(s + 1) * step_rows] = dot(chosen, pix[...]).astype(jnp.bfloat16)

    place_t = jnp.broadcast_to(place, (LANES, rows)).T
    part[...] = jnp.broadcast_to(piece, (LANES, rows)).T
    for s in range(packed_rows // LANES):
        index = lax.broadcasted_iota(jnp.int32, (rows, LANES), 1) + s * LANES
        pick[:, s * LANES:(s + 1) * LANES] = mask(place_t == index.astype(jnp.float32))

    for o in range(1, n_blk):
        bundle_copy(o, lax.rem(me + n_blk - o, n_blk)).wait_recv()

    together = min(groups, 4)
    lane = lax.broadcasted_iota(jnp.int32, (1, TILE), 1)
    seg = lane // width
    seg_rows = lax.broadcasted_iota(jnp.int32, (TILE, TILE), 0) // width
    seg_cols = lax.broadcasted_iota(jnp.int32, (TILE, TILE), 1) // width
    hold = TILE // (owned * width)
    half = lax.broadcasted_iota(jnp.int32, (1, LANES), 1) // width
    in_half = LANES // width
    row_of = lax.broadcasted_iota(jnp.int32, (cap, TILE), 0).astype(jnp.float32)
    energy_lane = lax.broadcasted_iota(jnp.int32, (1, LANES), 1)

    def group_spectra(g):
        return jnp.concatenate([spectra[g * hold + i] for i in range(hold)], axis=1)

    def solve(c, energy):
        for i in range(together):
            g = c * together + i
            both = group_spectra(g)
            gram = dot(both, both, ((0,), (0,))) + sum_weight
            gram = jnp.where(seg_rows == seg_cols, gram, 0.0)
            total = jnp.sum(jnp.abs(gram), axis=0, keepdims=True)
            step = jnp.zeros_like(total)
            for j in range(per):
                top = jnp.max(jnp.where(seg == j, total, 0.0), axis=1, keepdims=True)
                step = jnp.where(seg == j, 1.0 / top, step)
            high, low = split(gram * step)
            m_ref[i, 0:TILE] = high
            m_ref[i, TILE:2 * TILE] = high
            m_ref[i, 2 * TILE:3 * TILE] = low
            raw = dot(slots[pl.ds(g * per * cap, per * cap)], both)
            target = raw[0:cap]
            for j in range(1, per):
                target = jnp.where(seg == j, raw[j * cap:(j + 1) * cap], target)
            moved = step * (target + sum_weight)
            c_ref[i] = moved
            a_ref[i] = jnp.maximum(moved, 0.0)
        for _ in range(ITERS - 1):
            for i in range(together):
                state = a_ref[i]
                high, low = split(state)
                grad = dot(jnp.concatenate([high, low, high], axis=1), m_ref[i])
                a_ref[i] = jnp.maximum(state - grad + c_ref[i], 0.0)
        for i in range(together):
            g = c * together + i
            state = a_ref[i]
            high, low = split(state)
            packed[pl.ds(g * cap, cap)] = high
            packed[pl.ds(packed_rows + g * cap, cap)] = low
            tops = [counts[pl.ds(g * per + j, 1), :] for j in range(per)]
            spans = []
            for h in range(per // in_half):
                span = tops[h * in_half]
                for j in range(1, in_half):
                    span = jnp.where(half == j, tops[h * in_half + j], span)
                spans.append(span)
            kept = jnp.where(row_of < jnp.concatenate(spans, axis=1), state, 0.0)
            high, low = split(
                jnp.concatenate([jnp.where(seg == j, kept, 0.0) for j in range(per)], axis=0)
            )
            both = group_spectra(g)
            fitted = dot(high, both, ((1,), (1,))) + dot(low, both, ((1,), (1,)))
            misfit = slots[pl.ds(g * per * cap, per * cap)].astype(jnp.float32) - fitted
            square = misfit * misfit
            for j in range(per):
                column = jnp.sum(square[j * cap:(j + 1) * cap], axis=0, keepdims=True)
                value = jnp.sum(column, axis=1, keepdims=True)
                energy = jnp.where(energy_lane == g * per + j, value, energy)
        return energy

    energy = jnp.zeros((1, LANES), jnp.float32)
    if groups == together:
        energy = solve(0, energy)
    else:
        energy = lax.fori_loop(0, groups // together, solve, energy)
    scale = bands * rows * n_pix / count
    sums[my] = jnp.broadcast_to(energy * (1.0 / scale), sums.shape[1:])

    def energy_copy(o, which):
        return pltpu.make_async_remote_copy(
            src_ref=sums.at[which],
            dst_ref=sums.at[which],
            send_sem=esend_sem.at[o],
            recv_sem=erecv_sem.at[o],
            device_id=(me, lax.rem(my + o, n_pix)),
            device_id_type=MESH,
        )

    def put(r):
        cut = pl.ds(r * TILE, TILE)
        return pltpu.make_async_copy(out.at[cut], out_hbm.at[cut], out_sem.at[r])

    def unsort(r):
        cut = slice(r * TILE, (r + 1) * TILE)
        one = pick[cut]
        wide = dot(jnp.concatenate([one, one], axis=1), packed[...])
        where_ = part[cut]
        value = jnp.zeros((TILE, width), jnp.float32)
        for h in range(per // in_half):
            block = wide[:, h * LANES:(h + 1) * LANES]
            for j in range(in_half):
                shifted = block if j == 0 else pltpu.roll(block, LANES - j * width, 1)
                value = jnp.where(
                    where_[:, :width] == float(h * in_half + j), shifted[:, :width], value
                )
        out[cut] = value
        put(r).start()

    for r in range(rows // TILE):
        unsort(r)
        if r == 0:
            for o in range(1, n_pix):
                energy_copy(o, my).start()
    for o in range(1, n_pix):
        energy_copy(o, lax.rem(my + n_pix - o, n_pix)).wait_recv()
    total = sums[0]
    for i in range(1, n_pix):
        total = total + sums[i]
    energy_ref[...] = total[0:1, :count]
    for o in range(1, n_pix):
        energy_copy(o, my).wait_send()
    for o in range(1, n_blk):
        bundle_copy(o, me).wait_send()
    for r in range(rows // TILE):
        put(r).wait()


def per_device(pixels, bundles, assign):
    rows, bands = pixels.shape
    owned, _, width = bundles.shape
    n_blk, n_pix = lax.axis_size("blk"), lax.axis_size("pix")
    count = n_blk * owned
    cap = 2 * rows // count
    per = TILE // width
    groups = count // per
    together = min(groups, 4)
    packed_rows = groups * cap
    any_space = pl.BlockSpec(memory_space=pl.ANY)
    vmem = pl.BlockSpec(memory_space=pltpu.VMEM)
    return pl.pallas_call(
        functools.partial(kernel, (n_blk, n_pix)),
        out_shape=(
            jax.ShapeDtypeStruct((rows, width), jnp.float32),
            jax.ShapeDtypeStruct((1, count), jnp.float32),
        ),
        in_specs=[vmem, any_space, any_space],
        out_specs=(any_space, vmem),
        scratch_shapes=[
            pltpu.VMEM((rows, bands), jnp.bfloat16),
            pltpu.VMEM((owned, bands, width), jnp.bfloat16),
            pltpu.VMEM((n_blk, bands, owned * width), jnp.bfloat16),
            pltpu.VMEM((count * cap, bands), jnp.bfloat16),
            pltpu.VMEM((count, LANES), jnp.float32),
            pltpu.VMEM((rows, packed_rows), jnp.bfloat16),
            pltpu.VMEM((rows, LANES), jnp.float32),
            pltpu.VMEM((together, 3 * TILE, TILE), jnp.bfloat16),
            pltpu.VMEM((together, cap, TILE), jnp.float32),
            pltpu.VMEM((together, cap, TILE), jnp.float32),
            pltpu.VMEM((2 * packed_rows, TILE), jnp.bfloat16),
            pltpu.VMEM((rows, width), jnp.float32),
            pltpu.VMEM((n_pix, 8, LANES), jnp.float32),
            pltpu.SemaphoreType.DMA((2,)),
            pltpu.SemaphoreType.DMA((rows // TILE,)),
            pltpu.SemaphoreType.DMA((n_blk,)),
            pltpu.SemaphoreType.DMA((n_blk,)),
            pltpu.SemaphoreType.DMA((n_pix,)),
            pltpu.SemaphoreType.DMA((n_pix,)),
        ],
        compiler_params=pltpu.CompilerParams(collective_id=0, has_side_effects=True),
        name="unmix",
    )(assign.reshape(1, rows), pixels, bundles)


def solution(mesh):
    placed = (P(("blk", "pix"), None), P("blk", None, None), P(("blk", "pix"), None))
    return jax.shard_map(
        per_device,
        mesh=mesh,
        in_specs=placed,
        out_specs=(P(("blk", "pix"), None), P("blk", None)),
        check_vma=False,
    )
```

```python
import functools

import jax
import jax.numpy as jnp
from jax import lax
from jax.experimental import pallas as pl
from jax.experimental.pallas import tpu as pltpu
from jax.sharding import PartitionSpec as P

ITERS = 8
MESH = pl.DeviceIdType.MESH
LANES = 128
TILE = 256

sum_weight = 0.015625
ACROSS = ((1,), (1,))


def split(value):
    high = value.astype(jnp.bfloat16)
    low = (value - high.astype(jnp.float32)).astype(jnp.bfloat16)
    return high, low


def mask(cond):
    return jnp.where(cond, 1.0, 0.0).astype(jnp.bfloat16)


def dot(a, b, dims=((1,), (0,))):
    return lax.dot_general(a, b, (dims, ((), ())), preferred_element_type=jnp.float32)


def kernel(
    dims, label_ref, pix_hbm, bun_hbm, out_hbm, energy_ref,
    pix, spectra, slots, counts, pick, m_ref, c_ref, a_ref, packed, turned, out, sums,
    local_sem, out_sem, send_sem, recv_sem, esend_sem, erecv_sem,
):
    n_blk, n_pix, owned = dims
    me, my = lax.axis_index("blk"), lax.axis_index("pix")
    bands, rows = pix.shape
    piece_rows = bun_hbm.shape[0]
    width = piece_rows // owned
    count = n_blk * owned
    cap = 2 * rows // count
    per = TILE // width
    groups = count // per
    packed_rows = groups * cap
    hold = n_blk // groups
    together = min(groups, 4)
    z, y = me // hold, lax.rem(me, hold)

    def piece_at(device):
        return spectra.at[pl.ds(device * piece_rows, piece_rows)]

    get_bun = pltpu.make_async_copy(bun_hbm, piece_at(me), local_sem.at[0])
    get_pix = pltpu.make_async_copy(pix_hbm, pix, local_sem.at[1])
    get_bun.start()
    get_pix.start()

    barrier = pltpu.get_barrier_semaphore()
    for o in range(1, n_blk):
        pl.semaphore_signal(
            barrier, inc=1, device_id=(lax.rem(me + o, n_blk), my), device_id_type=MESH
        )
    for o in range(1, n_pix):
        pl.semaphore_signal(
            barrier, inc=1, device_id=(me, lax.rem(my + o, n_pix)), device_id_type=MESH
        )

    label = label_ref[...]
    kinds = lax.broadcasted_iota(jnp.int32, (count, TILE), 0)
    blocks = rows // TILE
    hot = [
        jnp.where(label[:, b * TILE:(b + 1) * TILE] == kinds, 1.0, 0.0) for b in range(blocks)
    ]
    upper = mask(
        lax.broadcasted_iota(jnp.int32, (TILE, TILE), 0)
        <= lax.broadcasted_iota(jnp.int32, (TILE, TILE), 1)
    )
    run = dot(jnp.concatenate(hot, axis=0).astype(jnp.bfloat16), upper)
    carry = jnp.zeros((count, 1), jnp.float32)
    ranks = []
    for b in range(blocks):
        here = run[b * count:(b + 1) * count]
        ranks.append(jnp.sum(hot[b] * (here + carry), axis=0, keepdims=True) - 1.0)
        carry = carry + here[:, TILE - 1:TILE]
    counts[...] = jnp.broadcast_to(carry, counts.shape)
    rank = jnp.concatenate(ranks, axis=1)
    shift = per.bit_length() - 1
    slot = label.astype(jnp.float32) * float(cap) + rank
    place = (label >> shift).astype(jnp.float32) * float(cap) + rank
    part = label & (per - 1)
    for s in range(packed_rows // LANES):
        index = lax.broadcasted_iota(jnp.int32, (LANES, rows), 0) + s * LANES
        pick[s * LANES:(s + 1) * LANES] = mask(place == index.astype(jnp.float32))

    get_bun.wait()
    pl.semaphore_wait(barrier, n_blk + n_pix - 2)

    def bundle_copy(dz, dy, which):
        peer = lax.rem(z + dz, groups) * hold + lax.rem(y + dy, hold)
        return pltpu.make_async_remote_copy(
            src_ref=piece_at(which),
            dst_ref=piece_at(which),
            send_sem=send_sem.at[dz * hold + dy],
            recv_sem=recv_sem.at[dz * hold + dy],
            device_id=(peer, my),
            device_id_type=MESH,
        )

    def arrived(dz):
        for dy in range(hold):
            if dz or dy:
                source = lax.rem(z + groups - dz, groups) * hold + lax.rem(y + hold - dy, hold)
                bundle_copy(dz, dy, source).wait_recv()

    order = sorted(range(groups), key=lambda dz: min(dz, groups - dz))
    others = [(dz, dy) for dz in order for dy in range(hold) if dz or dy]
    for dz, dy in others:
        bundle_copy(dz, dy, me).start()

    get_pix.wait()
    step_rows = 512
    for s in range(count * cap // step_rows):
        index = lax.broadcasted_iota(jnp.int32, (step_rows, rows), 0) + s * step_rows
        chosen = mask(slot == index.astype(jnp.float32))
        slots[s * step_rows:(s + 1) * step_rows] = dot(chosen, pix[...], ACROSS).astype(
            jnp.bfloat16
        )

    lane = lax.broadcasted_iota(jnp.int32, (1, TILE), 1)
    seg = lane // width
    seg_rows = lax.broadcasted_iota(jnp.int32, (TILE, TILE), 0) // width
    seg_cols = lax.broadcasted_iota(jnp.int32, (TILE, TILE), 1) // width
    half = lax.broadcasted_iota(jnp.int32, (1, LANES), 1) // width
    in_half = LANES // width
    row_of = lax.broadcasted_iota(jnp.int32, (cap, TILE), 0).astype(jnp.float32)
    energy_lane = lax.broadcasted_iota(jnp.int32, (1, LANES), 1)

    def group_spectra(g):
        return spectra[pl.ds(g * TILE, TILE)]

    def prepare(i, g):
        both = group_spectra(g)
        gram = dot(both, both, ACROSS) + sum_weight
        gram = jnp.where(seg_rows == seg_cols, gram, 0.0)
        total = jnp.sum(jnp.abs(gram), axis=0, keepdims=True)
        step = jnp.zeros_like(total)
        for j in range(per):
            top = jnp.max(jnp.where(seg == j, total, 0.0), axis=1, keepdims=True)
            step = jnp.where(seg == j, 1.0 / top, step)
        high, low = split(gram * step)
        m_ref[i, 0:TILE] = high
        m_ref[i, TILE:2 * TILE] = high
        m_ref[i, 2 * TILE:3 * TILE] = low
        raw = dot(slots[pl.ds(g * per * cap, per * cap)], both, ACROSS)
        target = raw[0:cap]
        for j in range(1, per):
            target = jnp.where(seg == j, raw[j * cap:(j + 1) * cap], target)
        moved = step * (target + sum_weight)
        c_ref[i] = moved
        a_ref[i] = jnp.maximum(moved, 0.0)

    def iterate(which):
        for _ in range(ITERS - 1):
            for i in which:
                state = a_ref[i]
                high, low = split(state)
                grad = dot(jnp.concatenate([high, low, high], axis=1), m_ref[i])
                a_ref[i] = jnp.maximum(state - grad + c_ref[i], 0.0)

    def finish(i, g, energy):
        state = a_ref[i]
        packed[pl.ds(g * cap, cap)] = state
        tops = [counts[pl.ds(g * per + j, 1), :] for j in range(per)]
        spans = []
        for h in range(per // in_half):
            span = tops[h * in_half]
            for j in range(1, in_half):
                span = jnp.where(half == j, tops[h * in_half + j], span)
            spans.append(span)
        kept = jnp.where(row_of < jnp.concatenate(spans, axis=1), state, 0.0)
        high, low = split(
            jnp.concatenate([jnp.where(seg == j, kept, 0.0) for j in range(per)], axis=0)
        )
        both = group_spectra(g)
        fitted = dot(high, both) + dot(low, both)
        misfit = slots[pl.ds(g * per * cap, per * cap)].astype(jnp.float32) - fitted
        square = misfit * misfit
        for j in range(per):
            column = jnp.sum(square[j * cap:(j + 1) * cap], axis=0, keepdims=True)
            value = jnp.sum(column, axis=1, keepdims=True)
            energy = jnp.where(energy_lane == g * per + j, value, energy)
        return energy

    energy = jnp.zeros((1, LANES), jnp.float32)
    if groups == together:
        numbers = [lax.rem(z + groups - dz, groups) for dz in order]
        for i, dz in enumerate(order):
            arrived(dz)
            prepare(i, numbers[i])
        iterate(range(groups))
        for i in range(groups):
            energy = finish(i, numbers[i], energy)
    else:
        for dz in order:
            arrived(dz)

        def chunk(c, energy):
            for i in range(together):
                prepare(i, c * together + i)
            iterate(range(together))
            for i in range(together):
                energy = finish(i, c * together + i, energy)
            return energy

        energy = lax.fori_loop(0, groups // together, chunk, energy)
    scale = bands * rows * n_pix / count
    sums[my] = jnp.broadcast_to(energy * (1.0 / scale), sums.shape[1:])

    def energy_copy(o, which):
        return pltpu.make_async_remote_copy(
            src_ref=sums.at[which],
            dst_ref=sums.at[which],
            send_sem=esend_sem.at[o],
            recv_sem=erecv_sem.at[o],
            device_id=(me, lax.rem(my + o, n_pix)),
            device_id_type=MESH,
        )

    high, low = split(packed[...].T)
    turned[0:TILE] = high
    turned[TILE:2 * TILE] = low
    for o in range(1, n_pix):
        energy_copy(o, my).start()

    def put(r):
        cut = pl.ds(r * TILE, TILE)
        return pltpu.make_async_copy(out.at[:, cut], out_hbm.at[:, cut], out_sem.at[r])

    for r in range(rows // TILE):
        cut = slice(r * TILE, (r + 1) * TILE)
        pair = dot(turned[...], pick[:, cut])
        wide = pair[:TILE] + pair[TILE:]
        which = part[:, cut]
        value = wide[0:width]
        for j in range(1, per):
            value = jnp.where(which == j, wide[j * width:(j + 1) * width], value)
        out[:, cut] = value
        put(r).start()

    for o in range(1, n_pix):
        energy_copy(o, lax.rem(my + n_pix - o, n_pix)).wait_recv()
    total = sums[0]
    for i in range(1, n_pix):
        total = total + sums[i]
    energy_ref[...] = total[0:1, :count]
    for o in range(1, n_pix):
        energy_copy(o, my).wait_send()
    for dz, dy in others:
        bundle_copy(dz, dy, me).wait_send()
    for r in range(rows // TILE):
        put(r).wait()


def per_device(pixels, bundles, assign):
    rows, bands = pixels.shape
    owned, _, width = bundles.shape
    n_blk, n_pix = lax.axis_size("blk"), lax.axis_size("pix")
    count = n_blk * owned
    cap = 2 * rows // count
    per = TILE // width
    groups = count // per
    together = min(groups, 4)
    packed_rows = groups * cap
    any_space = pl.BlockSpec(memory_space=pl.ANY)
    vmem = pl.BlockSpec(memory_space=pltpu.VMEM)
    abundances, energy = pl.pallas_call(
        functools.partial(kernel, (n_blk, n_pix, owned)),
        out_shape=(
            jax.ShapeDtypeStruct((width, rows), jnp.float32),
            jax.ShapeDtypeStruct((1, count), jnp.float32),
        ),
        in_specs=[vmem, any_space, any_space],
        out_specs=(any_space, vmem),
        scratch_shapes=[
            pltpu.VMEM((bands, rows), jnp.bfloat16),
            pltpu.VMEM((count * width, bands), jnp.bfloat16),
            pltpu.VMEM((count * cap, bands), jnp.bfloat16),
            pltpu.VMEM((count, LANES), jnp.float32),
            pltpu.VMEM((packed_rows, rows), jnp.bfloat16),
            pltpu.VMEM((together, 3 * TILE, TILE), jnp.bfloat16),
            pltpu.VMEM((together, cap, TILE), jnp.float32),
            pltpu.VMEM((together, cap, TILE), jnp.float32),
            pltpu.VMEM((packed_rows, TILE), jnp.float32),
            pltpu.VMEM((2 * TILE, packed_rows), jnp.bfloat16),
            pltpu.VMEM((width, rows), jnp.float32),
            pltpu.VMEM((n_pix, 8, LANES), jnp.float32),
            pltpu.SemaphoreType.DMA((2,)),
            pltpu.SemaphoreType.DMA((rows // TILE,)),
            pltpu.SemaphoreType.DMA((n_blk,)),
            pltpu.SemaphoreType.DMA((n_blk,)),
            pltpu.SemaphoreType.DMA((n_pix,)),
            pltpu.SemaphoreType.DMA((n_pix,)),
        ],
        compiler_params=pltpu.CompilerParams(collective_id=0, has_side_effects=True),
        name="unmix",
    )(
        assign.reshape(1, rows),
        pixels.T,
        bundles.transpose(0, 2, 1).reshape(owned * width, bands),
    )
    return abundances.T, energy


def solution(mesh):
    placed = (P(("blk", "pix"), None), P("blk", None, None), P(("blk", "pix"), None))
    return jax.shard_map(
        per_device,
        mesh=mesh,
        in_specs=placed,
        out_specs=(P(("blk", "pix"), None), P("blk", None)),
        check_vma=False,
    )
```

```python
import functools

import jax
import jax.numpy as jnp
from jax import lax
from jax.experimental import pallas as pl
from jax.experimental.pallas import tpu as pltpu
from jax.sharding import PartitionSpec as P

ITERS = 8
MESH = pl.DeviceIdType.MESH
LANES = 128
TILE = 256

sum_weight = 0.015625
ACROSS = ((1,), (1,))


def split(value):
    high = value.astype(jnp.bfloat16)
    low = (value - high.astype(jnp.float32)).astype(jnp.bfloat16)
    return high, low


def mask(cond):
    return jnp.where(cond, 1.0, 0.0).astype(jnp.bfloat16)


def dot(a, b, dims=((1,), (0,))):
    return lax.dot_general(a, b, (dims, ((), ())), preferred_element_type=jnp.float32)


def kernel(
    dims, label_ref, pix_hbm, bun_hbm, out_hbm, energy_ref,
    pix, own, spectra, slots, counts, pick, m_ref, c_ref, a_ref, packed, turned, out, sums,
    local_sem, out_sem, send_sem, recv_sem, esend_sem, erecv_sem,
):
    n_blk, n_pix, owned = dims
    me, my = lax.axis_index("blk"), lax.axis_index("pix")
    bands, rows = pix.shape
    piece_rows = bun_hbm.shape[0]
    width = piece_rows // owned
    count = n_blk * owned
    cap = 2 * rows // count
    per = TILE // width
    groups = count // per
    packed_rows = groups * cap
    hold = n_blk // groups
    together = min(groups, 4)
    z, y = me // hold, lax.rem(me, hold)

    def piece_at(device):
        return spectra.at[device]

    get_bun = pltpu.make_async_copy(bun_hbm, own, local_sem.at[0])
    get_pix = pltpu.make_async_copy(pix_hbm, pix, local_sem.at[1])
    get_bun.start()
    get_pix.start()

    barrier = pltpu.get_barrier_semaphore()
    for o in range(1, n_blk):
        pl.semaphore_signal(
            barrier, inc=1, device_id=(lax.rem(me + o, n_blk), my), device_id_type=MESH
        )
    for o in range(1, n_pix):
        pl.semaphore_signal(
            barrier, inc=1, device_id=(me, lax.rem(my + o, n_pix)), device_id_type=MESH
        )

    get_bun.wait()
    spectra[me] = own[...].astype(jnp.float32).T.astype(jnp.bfloat16)

    label = label_ref[...]
    kinds = lax.broadcasted_iota(jnp.int32, (count, TILE), 0)
    blocks = rows // TILE
    hot = [
        jnp.where(label[:, b * TILE:(b + 1) * TILE] == kinds, 1.0, 0.0) for b in range(blocks)
    ]
    upper = mask(
        lax.broadcasted_iota(jnp.int32, (TILE, TILE), 0)
        <= lax.broadcasted_iota(jnp.int32, (TILE, TILE), 1)
    )
    run = dot(jnp.concatenate(hot, axis=0).astype(jnp.bfloat16), upper)
    carry = jnp.zeros((count, 1), jnp.float32)
    ranks = []
    for b in range(blocks):
        here = run[b * count:(b + 1) * count]
        ranks.append(jnp.sum(hot[b] * (here + carry), axis=0, keepdims=True) - 1.0)
        carry = carry + here[:, TILE - 1:TILE]
    counts[...] = jnp.broadcast_to(carry, counts.shape)
    rank = jnp.concatenate(ranks, axis=1)
    shift = per.bit_length() - 1
    slot = label.astype(jnp.float32) * float(cap) + rank
    place = (label >> shift).astype(jnp.float32) * float(cap) + rank
    part = label & (per - 1)
    for s in range(packed_rows // LANES):
        index = lax.broadcasted_iota(jnp.int32, (LANES, rows), 0) + s * LANES
        pick[s * LANES:(s + 1) * LANES] = mask(place == index.astype(jnp.float32))

    pl.semaphore_wait(barrier, n_blk + n_pix - 2)

    def bundle_copy(dz, dy, which):
        peer = lax.rem(z + dz, groups) * hold + lax.rem(y + dy, hold)
        return pltpu.make_async_remote_copy(
            src_ref=piece_at(which),
            dst_ref=piece_at(which),
            send_sem=send_sem.at[dz * hold + dy],
            recv_sem=recv_sem.at[dz * hold + dy],
            device_id=(peer, my),
            device_id_type=MESH,
        )

    def arrived(dz):
        for dy in range(hold):
            if dz or dy:
                source = lax.rem(z + groups - dz, groups) * hold + lax.rem(y + hold - dy, hold)
                bundle_copy(dz, dy, source).wait_recv()

    order = sorted(range(groups), key=lambda dz: min(dz, groups - dz))
    others = [(dz, dy) for dz in order for dy in range(hold) if dz or dy]
    for dz, dy in others:
        bundle_copy(dz, dy, me).start()

    get_pix.wait()
    step_rows = 512
    for s in range(count * cap // step_rows):
        index = lax.broadcasted_iota(jnp.int32, (step_rows, rows), 0) + s * step_rows
        chosen = mask(slot == index.astype(jnp.float32))
        slots[s * step_rows:(s + 1) * step_rows] = dot(chosen, pix[...], ACROSS).astype(
            jnp.bfloat16
        )

    lane = lax.broadcasted_iota(jnp.int32, (1, TILE), 1)
    seg = lane // width
    seg_rows = lax.broadcasted_iota(jnp.int32, (TILE, TILE), 0) // width
    seg_cols = lax.broadcasted_iota(jnp.int32, (TILE, TILE), 1) // width
    half = lax.broadcasted_iota(jnp.int32, (1, LANES), 1) // width
    in_half = LANES // width
    row_of = lax.broadcasted_iota(jnp.int32, (cap, TILE), 0).astype(jnp.float32)
    energy_lane = lax.broadcasted_iota(jnp.int32, (1, LANES), 1)

    def group_spectra(g):
        return jnp.concatenate([spectra[g * hold + i] for i in range(hold)], axis=1)

    def prepare(i, g):
        both = group_spectra(g)
        gram = dot(both, both, ((0,), (0,))) + sum_weight
        gram = jnp.where(seg_rows == seg_cols, gram, 0.0)
        total = jnp.sum(jnp.abs(gram), axis=0, keepdims=True)
        step = jnp.zeros_like(total)
        for j in range(per):
            top = jnp.max(jnp.where(seg == j, total, 0.0), axis=1, keepdims=True)
            step = jnp.where(seg == j, 1.0 / top, step)
        high, low = split(gram * step)
        m_ref[i, 0:TILE] = high
        m_ref[i, TILE:2 * TILE] = high
        m_ref[i, 2 * TILE:3 * TILE] = low
        raw = dot(slots[pl.ds(g * per * cap, per * cap)], both)
        target = raw[0:cap]
        for j in range(1, per):
            target = jnp.where(seg == j, raw[j * cap:(j + 1) * cap], target)
        moved = step * (target + sum_weight)
        c_ref[i] = moved
        a_ref[i] = jnp.maximum(moved, 0.0)

    def iterate(which):
        for _ in range(ITERS - 1):
            for i in which:
                state = a_ref[i]
                high, low = split(state)
                grad = dot(jnp.concatenate([high, low, high], axis=1), m_ref[i])
                a_ref[i] = jnp.maximum(state - grad + c_ref[i], 0.0)

    def finish(i, g, energy):
        state = a_ref[i]
        packed[pl.ds(g * cap, cap)] = state
        tops = [counts[pl.ds(g * per + j, 1), :] for j in range(per)]
        spans = []
        for h in range(per // in_half):
            span = tops[h * in_half]
            for j in range(1, in_half):
                span = jnp.where(half == j, tops[h * in_half + j], span)
            spans.append(span)
        kept = jnp.where(row_of < jnp.concatenate(spans, axis=1), state, 0.0)
        high, low = split(
            jnp.concatenate([jnp.where(seg == j, kept, 0.0) for j in range(per)], axis=0)
        )
        both = group_spectra(g)
        fitted = dot(high, both, ACROSS) + dot(low, both, ACROSS)
        misfit = slots[pl.ds(g * per * cap, per * cap)].astype(jnp.float32) - fitted
        square = misfit * misfit
        for j in range(per):
            column = jnp.sum(square[j * cap:(j + 1) * cap], axis=0, keepdims=True)
            value = jnp.sum(column, axis=1, keepdims=True)
            energy = jnp.where(energy_lane == g * per + j, value, energy)
        return energy

    energy = jnp.zeros((1, LANES), jnp.float32)
    if groups == together:
        numbers = [lax.rem(z + groups - dz, groups) for dz in order]
        for i, dz in enumerate(order):
            arrived(dz)
            prepare(i, numbers[i])
        iterate(range(groups))
        for i in range(groups):
            energy = finish(i, numbers[i], energy)
    else:
        for dz in order:
            arrived(dz)

        def chunk(c, energy):
            for i in range(together):
                prepare(i, c * together + i)
            iterate(range(together))
            for i in range(together):
                energy = finish(i, c * together + i, energy)
            return energy

        energy = lax.fori_loop(0, groups // together, chunk, energy)
    scale = bands * rows * n_pix / count
    sums[my] = jnp.broadcast_to(energy * (1.0 / scale), sums.shape[1:])

    def energy_copy(o, which):
        return pltpu.make_async_remote_copy(
            src_ref=sums.at[which],
            dst_ref=sums.at[which],
            send_sem=esend_sem.at[o],
            recv_sem=erecv_sem.at[o],
            device_id=(me, lax.rem(my + o, n_pix)),
            device_id_type=MESH,
        )

    high, low = split(packed[...].T)
    turned[0:TILE] = high
    turned[TILE:2 * TILE] = low
    for o in range(1, n_pix):
        energy_copy(o, my).start()

    def put(r):
        cut = pl.ds(r * TILE, TILE)
        return pltpu.make_async_copy(out.at[:, cut], out_hbm.at[:, cut], out_sem.at[r])

    for r in range(rows // TILE):
        cut = slice(r * TILE, (r + 1) * TILE)
        pair = dot(turned[...], pick[:, cut])
        wide = pair[:TILE] + pair[TILE:]
        which = part[:, cut]
        value = wide[0:width]
        for j in range(1, per):
            value = jnp.where(which == j, wide[j * width:(j + 1) * width], value)
        out[:, cut] = value
        put(r).start()

    for o in range(1, n_pix):
        energy_copy(o, lax.rem(my + n_pix - o, n_pix)).wait_recv()
    total = sums[0]
    for i in range(1, n_pix):
        total = total + sums[i]
    energy_ref[...] = total[0:1, :count]
    for o in range(1, n_pix):
        energy_copy(o, my).wait_send()
    for dz, dy in others:
        bundle_copy(dz, dy, me).wait_send()
    for r in range(rows // TILE):
        put(r).wait()


def per_device(pixels, bundles, assign):
    rows, bands = pixels.shape
    owned, _, width = bundles.shape
    n_blk, n_pix = lax.axis_size("blk"), lax.axis_size("pix")
    count = n_blk * owned
    cap = 2 * rows // count
    per = TILE // width
    groups = count // per
    together = min(groups, 4)
    packed_rows = groups * cap
    any_space = pl.BlockSpec(memory_space=pl.ANY)
    vmem = pl.BlockSpec(memory_space=pltpu.VMEM)
    abundances, energy = pl.pallas_call(
        functools.partial(kernel, (n_blk, n_pix, owned)),
        out_shape=(
            jax.ShapeDtypeStruct((width, rows), jnp.float32),
            jax.ShapeDtypeStruct((1, count), jnp.float32),
        ),
        in_specs=[vmem, any_space, any_space],
        out_specs=(any_space, vmem),
        scratch_shapes=[
            pltpu.VMEM((bands, rows), jnp.bfloat16),
            pltpu.VMEM((owned * width, bands), jnp.bfloat16),
            pltpu.VMEM((n_blk, bands, owned * width), jnp.bfloat16),
            pltpu.VMEM((count * cap, bands), jnp.bfloat16),
            pltpu.VMEM((count, LANES), jnp.float32),
            pltpu.VMEM((packed_rows, rows), jnp.bfloat16),
            pltpu.VMEM((together, 3 * TILE, TILE), jnp.bfloat16),
            pltpu.VMEM((together, cap, TILE), jnp.float32),
            pltpu.VMEM((together, cap, TILE), jnp.float32),
            pltpu.VMEM((packed_rows, TILE), jnp.float32),
            pltpu.VMEM((2 * TILE, packed_rows), jnp.bfloat16),
            pltpu.VMEM((width, rows), jnp.float32),
            pltpu.VMEM((n_pix, 8, LANES), jnp.float32),
            pltpu.SemaphoreType.DMA((2,)),
            pltpu.SemaphoreType.DMA((rows // TILE,)),
            pltpu.SemaphoreType.DMA((n_blk,)),
            pltpu.SemaphoreType.DMA((n_blk,)),
            pltpu.SemaphoreType.DMA((n_pix,)),
            pltpu.SemaphoreType.DMA((n_pix,)),
        ],
        compiler_params=pltpu.CompilerParams(collective_id=0, has_side_effects=True),
        name="unmix",
    )(
        assign.reshape(1, rows),
        pixels.T,
        bundles.transpose(0, 2, 1).reshape(owned * width, bands),
    )
    return abundances.T, energy


def solution(mesh):
    placed = (P(("blk", "pix"), None), P("blk", None, None), P(("blk", "pix"), None))
    return jax.shard_map(
        per_device,
        mesh=mesh,
        in_specs=placed,
        out_specs=(P(("blk", "pix"), None), P("blk", None)),
        check_vma=False,
    )
```
